32 devices in a mesh: ctx: 16 (over z, x, core), head: 2 (over y).
Axes of the slice: x: 2, y: 2, z: 4, core: 2. Of those that a mesh axis runs over, the one named last changes fastest.
Arguments:
- queries: bfloat16 [2048, 2048], P('ctx', 'head'), may hold values from -160 to 160
- rotated_keys: bfloat16 [2048, 512], P('ctx', 'head'), may hold values from -6 to 6
- value_matrix: bfloat16 [2048, 512], P('ctx', 'head'), may hold values from -6 to 6
- doc_lengths: int32 [8], replicated, may hold values from 1 to 1536, 2048 in all
- scored: int32 [64], P('ctx'), may hold values from 0 to 127, as said below
- residual: bfloat16 [64, 4096], P('ctx', 'head'), may hold values from -18 to 18
- norm_gain: float32 [4096], P('head'), may hold values from 0.5 to 1.5
- out_weight: bfloat16 [2048, 4096], P('head'), may hold values from -0.5 to 0.5
- lm_weight: bfloat16 [4096, 128256], P('head', 'ctx'), may hold values from -0.40625 to 0.40625
- token_ids: int32 [64], replicated, may hold values from 0 to 128255
- old_logp: float32 [64], replicated, may hold values from -24 to -9
- advantage: float32 [64], replicated, may hold values from -3 to 3
Outputs:
- attended: bfloat16 [2048, 2048], P('ctx', 'head')
- log_probs: float32 [64], replicated
- token_loss: float32 [64], replicated
The draws below stay inside these ranges and needn't reach their ends.
Inputs may be any that keep to these rules, and one draw needn't show every extreme that they name: `scored`: each aligned block of 4 entries holds distinct increasing offsets. `doc_lengths`: the longest document has exactly three quarters of 2048 positions.
All inputs are finite; a program needn't handle non-finite values.
Results may differ from the reference program's by a relative error of at most 0.0065.
Values may be sent and summed in bfloat16 or wider, within the bound.
A program may use at most 128 MiB of HBM per device.

```python
import math
import jax
import jax.numpy as jnp
import numpy as np
from jax import lax

D = 4096
QUERY_HEADS = 16
KEY_VALUE_HEADS = 4
HEAD_SIZE = 128
V = 128256
TOK_DEV = 128
RESP_DEV = 4
DOCS = 8
PACKED_LENGTH = 2048
RESP = 64


def key_sample(key):
    drawn_sample = jax.random.normal(jax.random.fold_in(key, 12), (PACKED_LENGTH, KEY_VALUE_HEADS * HEAD_SIZE), jnp.float32)
    return jnp.clip(drawn_sample, -6.0, 6.0)


def draw_rotated_keys(key, part):
    sample = key_sample(key)
    return sample.astype(jnp.bfloat16)


def draw_queries(key, part):
    sample = 2.0 * jnp.clip(jax.random.normal(jax.random.fold_in(key, 11), (PACKED_LENGTH, QUERY_HEADS * HEAD_SIZE), jnp.float32), -6.0, 6.0)
    return sample.astype(jnp.bfloat16)


def draw_lm_weight(key, part):
    weight_scale = 3.0 * D ** (-0.5)
    sample = jnp.clip(jax.random.normal(jax.random.fold_in(key, 23), (D, V), jnp.float32), -6.0, 6.0) * weight_scale
    return sample.astype(jnp.bfloat16)


def column_scales():
    steps = jnp.arange(D, dtype=jnp.float32) / max(D - 1, 1)
    return jnp.exp(jnp.log(0.5) + steps * jnp.log(5.9))


def draw_residual(key, part):
    widths = column_scales()[None, :]
    sample = jnp.clip(jax.random.normal(jax.random.fold_in(key, 24), (RESP, D), jnp.float32), -6.0, 6.0) * widths
    return sample.astype(jnp.bfloat16)


def draw_scored(key, part):

    def one_block(block_index):
        picked = jax.random.permutation(jax.random.fold_in(key, block_index), TOK_DEV)[:RESP_DEV]
        return jnp.sort(picked)
    return jax.vmap(one_block)(jnp.arange(RESP // RESP_DEV)).reshape(RESP).astype(jnp.int32)


def with_ends(values, own_key, least, top_value):
    spot = [jax.random.randint(jax.random.fold_in(own_key, axis), (), 0, length) for axis, length in enumerate(values.shape)]
    main_axis = values.shape.index(max(values.shape))
    neighbour = spot[:main_axis] + [(spot[main_axis] + 1) % values.shape[main_axis]] + spot[main_axis + 1:]
    return values.at[tuple(spot)].set(least).at[tuple(neighbour)].set(top_value)


def block_scale(stream_key, shape, split, low, high):
    gain = 1.0
    for dim, blocks in split:
        heights = jax.random.uniform(jax.random.fold_in(jax.random.fold_in(stream_key, 6), dim), (blocks,), jnp.float32, low / len(split), high / len(split))
        gain = gain * jnp.repeat(jnp.exp(heights), shape[dim] // blocks).reshape((-1,) + (1,) * (len(shape) - 1 - dim))
    return gain


def skewed_wide(own_key, extent, number_of, lean):
    weights = [min(1 << octave, number_of + 1 - (1 << octave)) * (1 << 20) // math.isqrt((1 << octave) ** lean) + 1 for octave in range((number_of + 1).bit_length()) if 1 << octave <= number_of]
    width = 1 + sum(weights) // (1 << 30)
    table = np.cumsum(np.array([max(1, weight // width) for weight in weights]))
    lot = jax.random.randint(jax.random.fold_in(own_key, 1), extent, 0, int(table[len(weights) - 1]))
    start = jnp.left_shift(1, jnp.searchsorted(jnp.asarray(table, jnp.int32), lot, side="right").astype(jnp.int32))
    grade = start - 1 + jax.random.randint(jax.random.fold_in(own_key, 4), extent, 0, 1 << 30) % jnp.minimum(start, number_of + 1 - start)
    return jax.random.permutation(jax.random.fold_in(own_key, 2), number_of)[grade].astype(jnp.int32)


def length_profile(number_of, total, bound, skew):
    weights = [(1 << 20) // math.isqrt(grade ** skew) + 1 for grade in range(2, number_of + 1)]
    spare, holding = total - bound - (number_of - 1), [1] * (number_of - 1)
    while spare > 0:
        candidates = [i for i in range(number_of - 1) if holding[i] < bound]
        mass, budget = sum([weights[i] for i in candidates]), spare
        for i in candidates:
            addition = min(bound - holding[i], max(1, budget * weights[i] // mass), spare)
            holding[i] = holding[i] + addition
            spare = spare - addition
    return np.array([bound] + holding)


def ragged_sizes(own_key, count, total, limit, lean):
    if count == 2:
        one = jax.random.randint(own_key, (), max(1, total - limit), min(limit, total - 1) + 1)
        return jnp.stack([one, total - one])
    sizes = jnp.asarray(length_profile(count, total, limit, lean), jnp.int32)
    twos = (count - 1) // 2
    source_of, receiver = sizes[1:1 + 2 * twos:2], sizes[2:2 + 2 * twos:2]
    margin = jnp.minimum(source_of - 1, limit - receiver)
    shifted = jax.random.randint(jax.random.fold_in(own_key, 1), (twos,), 0, 1 << 20) % (margin + 1)
    sizes = sizes.at[1:1 + 2 * twos:2].set(source_of - shifted).at[2:2 + 2 * twos:2].set(receiver + shifted)
    return sizes[jax.random.permutation(jax.random.fold_in(own_key, 2), count)]


def centred(rng, extent, deviation, limit, pieces=(), kind=jnp.bfloat16):
    entries = deviation * jax.random.normal(rng, extent, jnp.float32)
    if pieces:
        entries = entries * block_scale(rng, extent, pieces, -0.22, 0.18)
    return jnp.clip(entries, -limit, limit).astype(kind)


def setup_inputs(seed: int = 0) -> dict:
    keys = jax.random.split(jax.random.key(seed), 13)
    return {
        "queries": draw_queries(jax.random.fold_in(keys[12], 71), 0),
        "rotated_keys": draw_rotated_keys(jax.random.fold_in(keys[12], 71), 0),
        "value_matrix": centred(keys[2], (PACKED_LENGTH, KEY_VALUE_HEADS * HEAD_SIZE), 1.0, 6.0, ((0, 16), (1, 2))),
        "doc_lengths": ragged_sizes(keys[3], DOCS, PACKED_LENGTH, 3 * PACKED_LENGTH // 4, 2).astype(jnp.int32),
        "scored": draw_scored(jax.random.fold_in(keys[12], 71), 0),
        "residual": draw_residual(jax.random.fold_in(keys[12], 71), 0),
        "norm_gain": jnp.clip(1.0 + 0.1 * jax.random.normal(keys[6], (D,), jnp.float32), 0.5, 1.5),
        "out_weight": centred(keys[7], (QUERY_HEADS * HEAD_SIZE, D), (QUERY_HEADS * HEAD_SIZE // 16) ** -0.5, 0.5, ((0, 2),)),
        "lm_weight": draw_lm_weight(jax.random.fold_in(keys[12], 71), 0),
        "token_ids": with_ends(skewed_wide(keys[9], (RESP,), V, 2), jax.random.fold_in(keys[9], 3), 0, V - 1).astype(jnp.int32),
        "old_logp": jnp.clip(jax.random.uniform(keys[10], (RESP,), jnp.float32, -24.0, -9.0), -24.0, -9.0),
        "advantage": centred(keys[11], (RESP,), 0.5, 3.0, (), jnp.float32),
    }


def doc_index(positions, doc_ends):
    return lax.optimization_barrier(jnp.sum((positions[:, None] >= doc_ends[None, :]).astype(jnp.int32), axis=1))

def reference(queries, rotated_keys, value_matrix, doc_lengths, scored, residual, norm_gain, out_weight, lm_weight, token_ids, old_logp, advantage):
    group_count = QUERY_HEADS // KEY_VALUE_HEADS
    doc_ends = jnp.cumsum(doc_lengths).astype(jnp.int32)
    key_pos = jnp.arange(PACKED_LENGTH, dtype=jnp.int32)
    key_doc = doc_index(key_pos, doc_ends)
    key_head_rows = rotated_keys.reshape(PACKED_LENGTH, KEY_VALUE_HEADS, HEAD_SIZE).astype(jnp.float32)
    value_head_rows = value_matrix.reshape(PACKED_LENGTH, KEY_VALUE_HEADS, HEAD_SIZE).astype(jnp.float32)
    query_matrix = min(256, PACKED_LENGTH)

    def one_block(offset):
        block_tile = lax.dynamic_slice_in_dim(queries, offset, query_matrix, 0)
        block_tile = block_tile.reshape(query_matrix, KEY_VALUE_HEADS, group_count, HEAD_SIZE).astype(jnp.float32)
        scores = jnp.einsum('qkgd,rkd->kgqr', block_tile, key_head_rows) * HEAD_SIZE ** (-0.5)
        query_pos = offset + jnp.arange(query_matrix, dtype=jnp.int32)
        allowed = (key_pos[None, :] <= query_pos[:, None]) & (key_doc[None, :] == doc_index(query_pos, doc_ends)[:, None])
        scores = jnp.where(allowed, scores, -1e+30)
        row_top = lax.optimization_barrier(jnp.max(scores, axis=-1, keepdims=True))
        weights = jnp.where(allowed, jnp.exp(scores - row_top), 0.0)
        row_total = lax.optimization_barrier(jnp.sum(weights, axis=-1, keepdims=True))
        probs = lax.optimization_barrier(weights.astype(jnp.bfloat16)).astype(jnp.float32)
        result = jnp.einsum('kgqr,rkd->kgqd', probs, value_head_rows) / row_total
        return jnp.transpose(result, (2, 0, 1, 3)).reshape(query_matrix, QUERY_HEADS * HEAD_SIZE).astype(jnp.bfloat16)
    offsets = jnp.arange(PACKED_LENGTH // query_matrix, dtype=jnp.int32) * query_matrix
    attended = lax.map(one_block, offsets).reshape(PACKED_LENGTH, QUERY_HEADS * HEAD_SIZE)
    positions = jnp.arange(RESP, dtype=jnp.int32) // RESP_DEV * TOK_DEV + scored
    chosen = jnp.take(attended, positions, axis=0)
    hidden = residual.astype(jnp.float32) + jnp.dot(chosen, out_weight, preferred_element_type=jnp.float32)
    mean_square = lax.optimization_barrier(jnp.mean(hidden * hidden, axis=1, keepdims=True))
    normed = (hidden * lax.rsqrt(mean_square + 1e-05) * norm_gain[None, :]).astype(jnp.bfloat16)
    logits = jnp.dot(normed, lm_weight, preferred_element_type=jnp.float32)
    row_top = lax.optimization_barrier(jnp.max(logits, axis=1))
    row_total = lax.optimization_barrier(jnp.sum(jnp.exp(logits - row_top[:, None]), axis=1))
    target = jnp.take_along_axis(logits, token_ids[:, None].astype(jnp.int32), axis=1)[:, 0]
    log_probs = target - row_top - jnp.log(row_total)
    ratio = jnp.exp(jnp.clip(log_probs - old_logp, -4.0, 4.0))
    token_loss = -jnp.minimum(ratio * advantage, jnp.clip(ratio, 0.8, 1.2) * advantage)
    return (attended, log_probs, token_loss)
```

```python
import functools

import jax
import jax.numpy as jnp
from jax import lax
from jax.experimental import pallas as pl
from jax.experimental.pallas import tpu as pltpu
from jax.sharding import PartitionSpec as P

HEAD_SIZE = 128
MESH = pl.DeviceIdType.MESH
MASKED = -1e30
QUAD = 4


def kernel(
    n,
    heads,
    tile,
    split,
    doc_ref,
    scored_ref,
    q_hbm,
    k_hbm,
    v_hbm,
    res_hbm,
    gain_hbm,
    wo_hbm,
    lm_hbm,
    ids_hbm,
    att_out,
    logp_ref,
    q_in,
    kv,
    qs,
    acc,
    top,
    tot,
    att,
    res,
    gain,
    wo,
    lm,
    ids,
    part,
    psend,
    precv,
    hid,
    u,
    rows32,
    rows16,
    lsend,
    lrecv,
    own,
    stats,
    in_sem,
    lm_sem,
    a_send,
    a_recv,
    x_send,
    x_recv,
    c_send,
    c_recv,
    y_send,
    y_recv,
    u_send,
    u_recv,
    d_send,
    d_recv,
    l_send,
    l_recv,
    s_send,
    s_recv,
):
    me = lax.axis_index("ctx")
    h = lax.axis_index("head")
    groups = n // QUAD
    g = me // QUAD
    r = me % QUAD
    rx = (r + 2) % QUAD
    rc = r + 1 - 2 * (r % 2)
    rd = (rc + 2) % QUAD
    base = me - r
    x_peer = base + rx
    c_peer = base + rc
    y_peer = 1 - h
    tok = q_in.shape[0]
    kv_heads = k_hbm.shape[1] // HEAD_SIZE
    per = q_in.shape[1] // k_hbm.shape[1]
    resp = u.shape[1]
    rows = n * resp
    half = res.shape[2]
    vocab = lm.shape[0]

    def local(src, dst, k):
        copy = pltpu.make_async_copy(src, dst, in_sem.at[k])
        copy.start()
        return copy

    def remote(src, dst, ss, rs, where):
        return pltpu.make_async_remote_copy(
            src_ref=src, dst_ref=dst, send_sem=ss, recv_sem=rs, device_id=where, device_id_type=MESH
        )

    def at(c):
        return {"ctx": c, "head": h}

    across = {"ctx": me, "head": y_peer}

    in_k = local(k_hbm, kv.at[me, 0], 0)
    in_v = local(v_hbm, kv.at[me, 1], 1)
    in_q = local(q_hbm, q_in, 2)
    in_res = local(res_hbm, res.at[h], 3)

    barrier = pltpu.get_barrier_semaphore()

    def greet(c, carry):
        for k in range(heads):
            @pl.when(jnp.logical_or(c != me, h != k))
            def _():
                pl.semaphore_signal(
                    barrier, inc=1, device_id={"ctx": c, "head": k}, device_id_type=MESH
                )
        return carry

    lax.fori_loop(0, n, greet, 0)
    in_gain = local(gain_hbm, gain, 4)
    in_ids = local(ids_hbm, ids, 5)
    in_wo = local(wo_hbm, wo, 8)
    in_k.wait()
    in_v.wait()
    in_res.wait()
    pl.semaphore_wait(barrier, n * heads - 1)

    later = g + 1 < groups

    def z_copy(src, p):
        piece = kv.at[src * QUAD + r, p]
        return remote(piece, piece, a_send.at[p, src], a_recv.at[p, src], at(me + QUAD))

    def x_copy(src, off, p):
        piece = kv.at[src * QUAD + off, p]
        return remote(piece, piece, x_send.at[p, src], x_recv.at[p, src], at(x_peer))

    def c_copy(src, off, kind, p):
        piece = kv.at[src * QUAD + off, p]
        return remote(piece, piece, c_send.at[kind, p, src], c_recv.at[kind, p, src], at(c_peer))

    def spread(src, p):
        @pl.when(later)
        def _():
            z_copy(src, p).start()

        x_copy(src, r, p).start()
        c_copy(src, r, 0, p).start()

    for p in range(2):
        spread(g, p)
    res_copy = remote(res.at[h], res.at[h], y_send.at[0], y_recv.at[0], across)
    res_copy.start()

    lm_rows = pl.cdiv(pl.cdiv(vocab, 8), 16) * 16
    lm_copies = []
    for k in range(pl.cdiv(vocab, lm_rows)):
        s = pl.ds(k * lm_rows, min(lm_rows, vocab - k * lm_rows))
        copy = pltpu.make_async_copy(lm_hbm.at[s], lm.at[s], lm_sem.at[k])
        copy.start()
        lm_copies.append(copy)

    in_q.wait()
    for hh in range(kv_heads * per):
        qs[hh // per, pl.ds((hh % per) * tok, tok), :] = q_in[:, hh * HEAD_SIZE : (hh + 1) * HEAD_SIZE]

    ends = [doc_ref[0]]
    for k in range(1, doc_ref.shape[0]):
        ends.append(ends[-1] + doc_ref[k])
    qpos = me * tok + lax.broadcasted_iota(jnp.int32, (per, tok, 1), 1).reshape(per * tok, 1)
    first = jnp.zeros_like(qpos)
    for e in ends:
        first = jnp.where(qpos >= e, e, first)

    width = QUAD * tok

    def attend(src, fresh):
        kpos = src * width + lax.broadcasted_iota(jnp.int32, (1, width), 1)
        allowed = jnp.logical_and(kpos <= qpos, kpos >= first)
        for kh in range(kv_heads):
            lanes = slice(kh * HEAD_SIZE, (kh + 1) * HEAD_SIZE)
            keys = kv[pl.ds(src * QUAD, QUAD), 0, :, lanes].reshape(width, HEAD_SIZE)
            vals = kv[pl.ds(src * QUAD, QUAD), 1, :, lanes].reshape(width, HEAD_SIZE)
            s = lax.dot_general(
                qs[kh], keys, (((1,), (1,)), ((), ())), preferred_element_type=jnp.float32
            ) * HEAD_SIZE ** (-0.5)
            s = jnp.where(allowed, s, MASKED)
            peak = jnp.max(s, axis=1, keepdims=True)
            if fresh:
                new = peak
            else:
                new = jnp.maximum(top[kh], peak)
            w = jnp.exp(s - new)
            total = jnp.sum(w, axis=1, keepdims=True)
            upd = jnp.dot(w.astype(jnp.bfloat16), vals, preferred_element_type=jnp.float32)
            if fresh:
                acc[kh] = upd
                tot[kh] = total
            else:
                fix = jnp.exp(top[kh] - new)
                acc[kh] = acc[kh] * fix + upd
                tot[kh] = tot[kh] * fix + total
            top[kh] = new

    def settle(src):
        for p in range(2):
            x_copy(src, rx, p).wait_recv()
            c_copy(src, rx, 1, p).start()
        for p in range(2):
            c_copy(src, rc, 0, p).wait_recv()
            c_copy(src, rd, 1, p).wait_recv()

    def pull(src):
        for p in range(2):
            z_copy(src, p).wait_recv()
            spread(src, p)

    @pl.when(g > 0)
    def _():
        pull(g - 1)

    settle(g)
    attend(g, True)

    def step(d, carry):
        @pl.when(d < g)
        def _():
            pull(g - d - 1)

        settle(g - d)
        attend(g - d, False)
        return carry

    lax.fori_loop(1, g + 1, step, 0)

    for kh in range(kv_heads):
        out = (acc[kh] / tot[kh]).astype(jnp.bfloat16)
        for j in range(per):
            hh = kh * per + j
            att[:, hh * HEAD_SIZE : (hh + 1) * HEAD_SIZE] = out[j * tok : (j + 1) * tok]
    att_copy = local(att, att_out, 9)

    pick = lax.broadcasted_iota(jnp.int32, (8, tok), 1)
    line = lax.broadcasted_iota(jnp.int32, (8, tok), 0)
    wanted = jnp.full((8, tok), -1, jnp.int32)
    for k in range(resp):
        wanted = jnp.where(line == k, scored_ref[k], wanted)
    onehot = jnp.where(pick == wanted, 1.0, 0.0).astype(jnp.bfloat16)
    chosen = jnp.dot(onehot, att[...], preferred_element_type=jnp.float32).astype(jnp.bfloat16)
    in_wo.wait()
    cols = 2048

    def project(t, carry):
        s = pl.ds(pl.multiple_of(t * cols, cols), cols)
        piece = jnp.dot(chosen, wo[:, s], preferred_element_type=jnp.float32)[:resp]
        part[:, s] = piece
        psend[:, s] = piece.astype(jnp.bfloat16)
        return carry

    lax.fori_loop(0, wo.shape[1] // cols, project, 0)
    p_copy = remote(psend, precv, y_send.at[1], y_recv.at[1], across)
    p_copy.start()
    in_gain.wait()
    in_ids.wait()
    ids_col = jnp.transpose(
        jnp.broadcast_to(ids[...].astype(jnp.float32), (128, rows))
    )[:, 0:1].astype(jnp.int32)
    res_copy.wait()
    p_copy.wait()
    squares = jnp.zeros((resp, 1), jnp.float32)
    for k in range(heads):
        s = slice(k * half, (k + 1) * half)
        value = res[k].astype(jnp.float32) + (part[:, s] + precv[:, s].astype(jnp.float32))
        hid[k] = value
        squares = squares + jnp.sum(value * value, axis=1, keepdims=True)
    normed = hid[h] * lax.rsqrt(squares / (half * heads) + 1e-05) * gain[...]
    u[me] = normed.astype(jnp.bfloat16)

    core = me % 2
    mate = me + 1 - 2 * core
    chips = n // 2
    chip = me // 2

    def u_copy(c, dst):
        b = c * 2 + core
        return remote(u.at[b], u.at[b], u_send.at[dst], u_recv.at[c], at(dst * 2 + core))

    def d_copy(c, side):
        b = c * 2 + side
        return remote(u.at[b], u.at[b], d_send.at[c], d_recv.at[c], at(mate))

    def u_start(k, carry):
        u_copy(chip, (chip + k) % chips).start()
        return carry

    lax.fori_loop(1, chips, u_start, 0)
    d_copy(chip, core).start()

    def u_pass(k, carry):
        c = (chip + k) % chips
        u_copy(c, 0).wait_recv()
        d_copy(c, core).start()
        return carry

    lax.fori_loop(1, chips, u_pass, 0)

    def u_take(c, carry):
        d_copy(c, 1 - core).wait_recv()
        rows32[c, 0:resp, :] = u[2 * c].astype(jnp.float32)
        rows32[c, resp : 2 * resp, :] = u[2 * c + 1].astype(jnp.float32)
        return carry

    lax.fori_loop(0, chips, u_take, 0)
    rows16[...] = rows32[...].reshape(rows, half).astype(jnp.bfloat16)
    for copy in lm_copies:
        copy.wait()

    full = (vocab - split) // tile
    tails = (split - full * tile, vocab - split - full * tile)

    def l_copy(t):
        return remote(lsend.at[t], lrecv.at[t], l_send.at[t], l_recv.at[t], across)

    def columns(side, t):
        return pl.ds(pl.multiple_of(side * split + t * tile, 128), tile)

    def dot_columns(s):
        return lax.dot_general(
            rows16[...], lm[s, :], (((1,), (1,)), ((), ())), preferred_element_type=jnp.float32
        )

    def far(t, carry):
        lsend[t] = dot_columns(columns(y_peer, t)).astype(jnp.bfloat16)
        l_copy(t).start()
        return carry

    lax.fori_loop(0, full, far, 0)
    for k in range(2):
        if tails[k]:
            @pl.when(y_peer == k)
            def _():
                start = k * split + full * tile
                lsend[full, :, 0 : tails[k]] = dot_columns(slice(start, start + tails[k])).astype(jnp.bfloat16)
    if max(tails):
        l_copy(full).start()

    def near(t, carry):
        own[t] = dot_columns(columns(h, t))
        return carry

    lax.fori_loop(0, full, near, 0)
    for k in range(2):
        if tails[k]:
            @pl.when(h == k)
            def _():
                start = k * split + full * tile
                own[full, :, 0 : tails[k]] = dot_columns(slice(start, start + tails[k]))

    first_id = me * vocab + h * split
    last_tail = jnp.where(h == 0, tails[0], tails[1])

    def fold(t, state, limit):
        peak, total, target = state
        l_copy(t).wait_recv()
        z = own[t] + lrecv[t].astype(jnp.float32)
        lane = lax.broadcasted_iota(jnp.int32, (rows, tile), 1)
        if limit is not None:
            z = jnp.where(lane < limit, z, MASKED)
        hit = lane == ids_col - (first_id + t * tile)
        if limit is not None:
            hit = jnp.logical_and(hit, lane < limit)
        else:
            pass
        target = target + jnp.sum(jnp.where(hit, z, 0.0), axis=1, keepdims=True)
        new = jnp.maximum(peak, jnp.max(z, axis=1, keepdims=True))
        total = total * jnp.exp(peak - new) + jnp.sum(jnp.exp(z - new), axis=1, keepdims=True)
        return new, total, target

    state = (
        jnp.full((rows, 1), MASKED, jnp.float32),
        jnp.zeros((rows, 1), jnp.float32),
        jnp.zeros((rows, 1), jnp.float32),
    )
    state = lax.fori_loop(0, full, lambda t, c: fold(t, c, None), state)
    if max(tails):
        state = fold(full, state, last_tail)
    peak, total, target = state

    lane = lax.broadcasted_iota(jnp.int32, (rows, 128), 1)
    block = jnp.where(lane == 0, peak, jnp.where(lane == 1, total, jnp.where(lane == 2, target, 0.0)))
    flat = me * heads + h
    stats[flat] = jnp.transpose(block)[0:8]

    def s_copy(src, dst):
        return remote(
            stats.at[src],
            stats.at[src],
            s_send.at[dst],
            s_recv.at[src],
            {"ctx": dst // heads, "head": dst % heads},
        )

    everyone = n * heads

    def s_start(k, carry):
        s_copy(flat, (flat + k) % everyone).start()
        return carry

    lax.fori_loop(1, everyone, s_start, 0)

    def g_end(src, carry):
        for p in range(2):
            @pl.when(later)
            def _():
                z_copy(src, p).wait_send()

            x_copy(src, r, p).wait_send()
            c_copy(src, r, 0, p).wait_send()
            c_copy(src, rx, 1, p).wait_send()
        return carry

    lax.fori_loop(0, g + 1, g_end, 0)

    def u_end(k, carry):
        u_copy(chip, (chip + k) % chips).wait_send()
        return carry

    lax.fori_loop(1, chips, u_end, 0)

    def d_end(c, carry):
        d_copy(c, core).wait_send()
        return carry

    lax.fori_loop(0, chips, d_end, 0)

    def l_end(t, carry):
        l_copy(t).wait_send()
        return carry

    lax.fori_loop(0, full + (1 if max(tails) else 0), l_end, 0)
    att_copy.wait()

    def s_wait(k, carry):
        s_copy((flat + k) % everyone, 0).wait_recv()
        return carry

    lax.fori_loop(1, everyone, s_wait, 0)
    every = stats[...]
    peaks, totals, targets = every[:, 0:1, :], every[:, 1:2, :], every[:, 2:3, :]
    best = jnp.max(peaks, axis=0)
    total = jnp.sum(totals * jnp.exp(peaks - best[None]), axis=0)
    lead = jnp.sum(targets, axis=0) - best
    logp_ref[0:1, :] = lead
    logp_ref[1:2, :] = total

    def s_end(k, carry):
        s_copy(flat, (flat + k) % everyone).wait_send()
        return carry

    lax.fori_loop(1, everyone, s_end, 0)


def per_device(
    n,
    heads,
    queries,
    rotated_keys,
    value_matrix,
    doc_lengths,
    scored,
    residual,
    norm_gain,
    out_weight,
    lm_weight,
    token_ids,
    old_logp,
    advantage,
):
    tok, feats = queries.shape
    kv_feats = rotated_keys.shape[1]
    kv_heads = kv_feats // HEAD_SIZE
    per = feats // kv_feats
    resp = scored.shape[0]
    rows = n * resp
    half = residual.shape[1]
    width = half * heads
    depth, vocab = lm_weight.shape
    tile = 512
    split = pl.cdiv(pl.cdiv(vocab, 2), tile) * tile
    tiles = pl.cdiv(split, tile)
    groups = n // QUAD
    chips = n // 2
    bf16, f32 = jnp.bfloat16, jnp.float32
    vm, dma = pltpu.VMEM, pltpu.SemaphoreType.DMA
    hbm = pl.BlockSpec(memory_space=pl.ANY)
    smem = pl.BlockSpec(memory_space=pltpu.SMEM)
    vmem = pl.BlockSpec(memory_space=pltpu.VMEM)
    attended, pair = pl.pallas_call(
        functools.partial(kernel, n, heads, tile, split),
        out_shape=(
            jax.ShapeDtypeStruct((tok, feats), bf16),
            jax.ShapeDtypeStruct((2, rows), f32),
        ),
        in_specs=[smem, smem] + [hbm] * 8,
        out_specs=(hbm, vmem),
        scratch_shapes=[
            vm((tok, feats), bf16),
            vm((n, 2, tok, kv_feats), bf16),
            vm((kv_heads, per * tok, HEAD_SIZE), bf16),
            vm((kv_heads, per * tok, HEAD_SIZE), f32),
            vm((kv_heads, per * tok, 1), f32),
            vm((kv_heads, per * tok, 1), f32),
            vm((tok, feats), bf16),
            vm((heads, resp, half), bf16),
            vm((1, half), f32),
            vm(out_weight.shape, bf16),
            vm((vocab, depth), bf16),
            vm((1, rows), jnp.int32),
            vm((resp, width), f32),
            vm((resp, width), bf16),
            vm((resp, width), bf16),
            vm((heads, resp, half), f32),
            vm((n, resp, half), bf16),
            vm((chips, 2 * resp, half), f32),
            vm((rows, half), bf16),
            vm((tiles, rows, tile), bf16),
            vm((tiles, rows, tile), bf16),
            vm((tiles, rows, tile), f32),
            vm((n * heads, 8, rows), f32),
            dma((10,)),
            dma((8,)),
            dma((2, groups)),
            dma((2, groups)),
            dma((2, groups)),
            dma((2, groups)),
            dma((2, 2, groups)),
            dma((2, 2, groups)),
            dma((2,)),
            dma((2,)),
            dma((chips,)),
            dma((chips,)),
            dma((chips,)),
            dma((chips,)),
            dma((tiles,)),
            dma((tiles,)),
            dma((n * heads,)),
            dma((n * heads,)),
        ],
        compiler_params=pltpu.CompilerParams(
            collective_id=0, has_side_effects=True, vmem_limit_bytes=67043328 - (1 << 20)
        ),
    )(
        doc_lengths,
        scored,
        queries,
        rotated_keys,
        value_matrix,
        residual,
        norm_gain.reshape(1, half),
        out_weight,
        lm_weight.T,
        token_ids.reshape(1, rows),
    )
    log_probs = pair[0] - jnp.log(pair[1])
    ratio = jnp.exp(jnp.clip(log_probs - old_logp, -4.0, 4.0))
    token_loss = -jnp.minimum(ratio * advantage, jnp.clip(ratio, 0.8, 1.2) * advantage)
    return attended, log_probs, token_loss


def solution(mesh):
    return jax.shard_map(
        functools.partial(per_device, mesh.shape["ctx"], mesh.shape["head"]),
        mesh=mesh,
        in_specs=(
            P("ctx", "head"),
            P("ctx", "head"),
            P("ctx", "head"),
            P(),
            P("ctx"),
            P("ctx", "head"),
            P("head"),
            P("head", None),
            P("head", "ctx"),
            P(),
            P(),
            P(),
        ),
        out_specs=(P("ctx", "head"), P(), P()),
        check_vma=False,
    )
```
